512 devices in a mesh: groups: 2 (over y), seq: 32 (over z), head: 8 (over x, core).
Axes of the slice: x: 4, y: 2, z: 32, core: 2. Of those that a mesh axis runs over, the one named last changes fastest.
The devices are a block of a 4x16x32 slice.
Arguments:
- residual: bfloat16 [8192, 2048], P(('groups', 'seq')), parts along dimension 0, may hold values from -6 to 6
- query_in: bfloat16 [8192, 2048], P(('groups', 'seq'), 'head'), parts along dimension 0, may hold values from -6 to 6
- key_in: bfloat16 [8192, 2048], P(('groups', 'seq'), 'head'), parts along dimension 0, may hold values from -6 to 6
- value_in: bfloat16 [8192, 4096], P(('groups', 'seq'), 'head'), parts along dimension 0, may hold values from -6 to 6
- gating_in: bfloat16 [8192, 4096], P(('groups', 'seq'), 'head'), parts along dimension 0, may hold values from -6 to 6
- beta_logit: float32 [8192, 32], P(('groups', 'seq'), 'head'), parts along dimension 0, may hold values from -12 to 2
- decay_logit: float32 [8192, 32], P(('groups', 'seq'), 'head'), parts along dimension 0, may hold values from -16 to 1
- seq_length: int32 [2], P('groups'), parts along dimension 0, may hold values from 2048 to 4096
- conv_query: float32 [4, 2048], P(None, 'head'), may hold values from -3 to 3
- conv_key: float32 [4, 2048], P(None, 'head'), may hold values from -3 to 3
- conv_value: float32 [4, 4096], P(None, 'head'), may hold values from -3 to 3
- decay_rate: float32 [32], P('head'), may hold values from 0.5 to 136
- norm_gain: float32 [128], replicated, may hold values from 0.1 to 1.9
- out_weight: bfloat16 [4096, 2048], P('head'), may hold values from -0.09375 to 0.09375
- attn_gain: float32 [2048], replicated, may hold values from 0.1 to 1.9
- query_weight: bfloat16 [2048, 8192], P('seq', 'head'), may hold values from -1 to 1
- key_value_weight: bfloat16 [2048, 1024], P('seq'), may hold values from -10 to 10
Outputs:
- hidden_out: bfloat16 [8192, 2048], P(('groups', 'seq')), parts along dimension 0
- attention_out: bfloat16 [8192, 4096], P(('groups', 'seq'), 'head'), parts along dimension 0
The draws below stay inside these ranges and needn't reach their ends.
There are 2 independent parts, one for each index of `groups`. The reference program is written for one: setup_inputs(seed, part) draws one part's arguments, and reference() takes and returns one part's arrays. A program takes and returns all parts, laid end to end along the dimension named above; an argument that names none is the same for every part. Nothing has to cross between parts.
All inputs are finite; a program needn't handle non-finite values.
Results may differ from the reference program's by a relative error of at most 0.02.
The reference program's roundings to bfloat16 on the way count: a program that leaves them out, or rounds other values in their place, can miss the bound.
Values may be sent and summed in bfloat16 or wider, within the bound.
A program may use at most 128 MiB of HBM per device.

```python
import math
import jax
import jax.numpy as jnp
from jax import lax

MODEL_WIDTH = 2048
HK = 16
HV = 32
DK = 128
DV = 128
QUERY_HEADS = 16
KEY_VALUE_HEADS = 2
HEAD_WIDTH = 256
CONV = 4
TOK_DEV = 128
SEQUENCE_LENGTH = 4096


def weight_pair(key):
    bound = 6.0 / math.sqrt(MODEL_WIDTH)
    first_matrix = jax.random.normal(jax.random.fold_in(key, 11), (MODEL_WIDTH, QUERY_HEADS * 2 * HEAD_WIDTH), jnp.float32) / math.sqrt(MODEL_WIDTH)
    first_matrix = jnp.clip(first_matrix, -bound, bound)
    second_matrix = jax.random.normal(jax.random.fold_in(key, 12), (MODEL_WIDTH, 2 * KEY_VALUE_HEADS * HEAD_WIDTH), jnp.float32) / math.sqrt(MODEL_WIDTH)
    second_matrix = jnp.clip(second_matrix, -bound, bound)
    return (first_matrix, second_matrix)


def draw_query_weight(key, part):
    return weight_pair(key)[0].astype(jnp.bfloat16)


def draw_key_value_weight(key, part):
    return weight_pair(key)[1].astype(jnp.bfloat16)


def draw_beta_logit(key, part):
    token_places = jnp.arange(SEQUENCE_LENGTH, dtype=jnp.int32)
    stretch_length = 3 * TOK_DEV
    stretch_total = SEQUENCE_LENGTH // stretch_length + 1
    quiet_table = jax.random.randint(jax.random.fold_in(key, 32), (stretch_total, HV), 0, 2)
    quiet_rows = quiet_table[token_places // stretch_length]
    active = jax.random.uniform(jax.random.fold_in(key, 31), (SEQUENCE_LENGTH, HV), jnp.float32, -2.5, 1.5)
    silent = jax.random.uniform(jax.random.fold_in(key, 33), (SEQUENCE_LENGTH, HV), jnp.float32, -12.0, -10.0)
    return jnp.where(quiet_rows == 1, silent, active)


def draw_decay_logit(key, part):
    token_places = jnp.arange(SEQUENCE_LENGTH, dtype=jnp.int32)
    slab_total = SEQUENCE_LENGTH // TOK_DEV
    slab_offset = jax.random.uniform(jax.random.fold_in(key, 24), (slab_total, HV), jnp.float32, -2.0, 1.0)
    starting_shift = -math.log(SEQUENCE_LENGTH) + jax.random.uniform(jax.random.fold_in(key, 21), (SEQUENCE_LENGTH, HV), jnp.float32, -1.5, 1.5)
    starting_shift = starting_shift + slab_offset[token_places // TOK_DEV]
    location_entries = jax.random.randint(jax.random.fold_in(key, 22), (3, HV), 0, SEQUENCE_LENGTH)
    contiguous_lines = jnp.any(token_places[:, None, None] == location_entries[None], axis=1)
    threshold_amount = jax.random.uniform(jax.random.fold_in(key, 23), (SEQUENCE_LENGTH, HV), jnp.float32, 0.0, 1.0)
    return jnp.where(contiguous_lines, threshold_amount, starting_shift)


def block_levels(own_key, shape, split, smallest, top_value):
    loudness = 1.0
    for dim, parts in split:
        draws = jax.random.uniform(jax.random.fold_in(jax.random.fold_in(own_key, 6), dim), (parts,), jnp.float32, smallest / len(split), top_value / len(split))
        loudness = loudness * jnp.repeat(jnp.exp(draws), shape[dim] // parts).reshape((-1,) + (1,) * (len(shape) - 1 - dim))
    return loudness


def gaussian(own_key, shape, deviation, most, shards=(), kind=jnp.bfloat16):
    result = jax.random.normal(own_key, shape, jnp.float32) * deviation
    if len(shards) > 0:
        result = block_levels(own_key, shape, shards, -0.22, 0.18) * result
    return jnp.clip(result, min=-most, max=most).astype(kind)


def setup_inputs(seed: int = 0, part: int = 0) -> dict:
    keys = jax.random.split(jax.random.key(seed), 18)
    own_keys = jax.random.split(jax.random.fold_in(keys[17], part), 18)
    return {
        "residual": gaussian(own_keys[0], (SEQUENCE_LENGTH, MODEL_WIDTH), 1.0, 6.0, ((0, 32),)),
        "query_in": gaussian(own_keys[1], (SEQUENCE_LENGTH, HK * DK), 1.0, 6.0, ((0, 32), (1, 8))),
        "key_in": gaussian(own_keys[2], (SEQUENCE_LENGTH, HK * DK), 1.0, 6.0, ((0, 32), (1, 8))),
        "value_in": gaussian(own_keys[3], (SEQUENCE_LENGTH, HV * DV), 1.0, 6.0, ((0, 32), (1, 8))),
        "gating_in": gaussian(own_keys[4], (SEQUENCE_LENGTH, HV * DV), 1.0, 6.0, ((0, 32), (1, 8))),
        "beta_logit": draw_beta_logit(jax.random.fold_in(jax.random.fold_in(keys[17], part), 71), part),
        "decay_logit": draw_decay_logit(jax.random.fold_in(jax.random.fold_in(keys[17], part), 71), part),
        "seq_length": jax.random.randint(own_keys[7], (1,), SEQUENCE_LENGTH // 2, SEQUENCE_LENGTH + 1).astype(jnp.int32),
        "conv_query": gaussian(keys[8], (CONV, HK * DK), 0.5, 3.0, ((1, 8),), jnp.float32),
        "conv_key": gaussian(keys[9], (CONV, HK * DK), 0.5, 3.0, ((1, 8),), jnp.float32),
        "conv_value": gaussian(keys[10], (CONV, HV * DV), 0.5, 3.0, ((1, 8),), jnp.float32),
        "decay_rate": jnp.clip(jnp.exp(math.log(136.0) - 5.605802 * jax.random.uniform(keys[11], (HV,), jnp.float32) ** block_levels(keys[11], (HV,), ((0, 8),), -0.2, 0.2)), 0.5, 136.0),
        "norm_gain": jnp.clip(1.0 + 0.18 * jax.random.normal(keys[12], (DV,), jnp.float32), 0.1, 1.9),
        "out_weight": gaussian(keys[13], (HV * DV, MODEL_WIDTH), (HV * DV) ** -0.5, 0.09375, ((0, 8),)),
        "attn_gain": jnp.clip(1.0 + 0.18 * jax.random.normal(keys[14], (MODEL_WIDTH,), jnp.float32), 0.1, 1.9),
        "query_weight": draw_query_weight(jax.random.fold_in(keys[17], 71), part),
        "key_value_weight": draw_key_value_weight(jax.random.fold_in(keys[17], 71), part),
    }


EPSILON = 1e-06
NEGATIVE = -1e+30

def causal_conv(inputs, kernel):
    widened = inputs.astype(jnp.float32)
    padded = jnp.concatenate([jnp.zeros((CONV - 1, widened.shape[1]), jnp.float32), widened], 0)
    summed = jnp.zeros_like(widened)
    for offset in range(CONV):
        summed = summed + kernel[offset] * padded[offset:offset + widened.shape[0]]
    return jax.nn.silu(summed)

def unit_rows(tensor):
    return tensor / jnp.sqrt(lax.optimization_barrier(jnp.sum(tensor * tensor, -1, keepdims=True)) + EPSILON)

def reference(residual, query_in, key_in, value_in, gating_in, beta_logit, decay_logit, seq_length, conv_query, conv_key, conv_value, decay_rate, norm_gain, out_weight, attn_gain, query_weight, key_value_weight):
    highest_index = lax.Precision.HIGHEST
    positions = jnp.arange(SEQUENCE_LENGTH, dtype=jnp.int32)
    length_now = seq_length[0].astype(jnp.int32)
    alive_mask = (positions < length_now).astype(jnp.float32)
    queries = unit_rows(causal_conv(query_in, conv_query).reshape(SEQUENCE_LENGTH, HK, DK)) * DK ** (-0.5)
    keyset = unit_rows(causal_conv(key_in, conv_key).reshape(SEQUENCE_LENGTH, HK, DK))
    values = causal_conv(value_in, conv_value).reshape(SEQUENCE_LENGTH, HV, DV)
    queries = jnp.repeat(queries, HV // HK, axis=1)
    keyset = jnp.repeat(keyset, HV // HK, axis=1)
    betas = jax.nn.sigmoid(beta_logit) * alive_mask[:, None]
    log_decay = -decay_rate[None, :] * jax.nn.softplus(decay_logit) * alive_mask[:, None]

    def advance(recurrent_state, inputs):
        current_query, current_key, value_now, beta_now, decay_now = inputs
        recurrent_state = jnp.exp(decay_now)[:, None, None] * recurrent_state
        prediction = jnp.einsum('ino,in->io', recurrent_state, current_key, precision=highest_index)
        recurrent_state = recurrent_state + beta_now[:, None, None] * current_key[:, :, None] * (value_now - prediction)[:, None, :]
        return (recurrent_state, jnp.einsum('ino,in->io', recurrent_state, current_query, precision=highest_index))
    initial = jnp.zeros((HV, DK, DV), jnp.float32)
    _, outputs = lax.scan(advance, initial, (queries, keyset, values, betas, log_decay))
    gating = gating_in.astype(jnp.float32).reshape(SEQUENCE_LENGTH, HV, DV)
    scaled = outputs * lax.rsqrt(lax.optimization_barrier(jnp.mean(outputs * outputs, -1, keepdims=True)) + EPSILON)
    gated = (scaled * norm_gain * jax.nn.silu(gating)).astype(jnp.bfloat16).reshape(SEQUENCE_LENGTH, HV * DV)
    summed = jnp.dot(gated, out_weight, preferred_element_type=jnp.float32)
    hidden_out = (residual.astype(jnp.float32) + summed).astype(jnp.bfloat16)
    widened = hidden_out.astype(jnp.float32)
    normalized = (widened * lax.rsqrt(lax.optimization_barrier(jnp.mean(widened * widened, -1, keepdims=True)) + EPSILON) * attn_gain).astype(jnp.bfloat16)
    projected = jnp.dot(normalized, query_weight, preferred_element_type=jnp.float32).reshape(SEQUENCE_LENGTH, QUERY_HEADS, 2, HEAD_WIDTH)
    queries_att = projected[:, :, 0].astype(jnp.bfloat16)
    gating_att = projected[:, :, 1]
    key_value_full = jnp.dot(normalized, key_value_weight, preferred_element_type=jnp.float32).reshape(SEQUENCE_LENGTH, 2, KEY_VALUE_HEADS, HEAD_WIDTH).astype(jnp.bfloat16)
    group_width = QUERY_HEADS // KEY_VALUE_HEADS
    key_heads = jnp.repeat(key_value_full[:, 0].transpose(1, 0, 2), group_width, 0)
    value_heads = jnp.repeat(key_value_full[:, 1].transpose(1, 0, 2), group_width, 0)
    visible = (positions[None, :] <= positions[:, None]) & (positions[None, :] < length_now)

    def attend_head(operands):
        head_query, head_key, head_value = operands
        scores = jnp.dot(head_query, head_key.T, preferred_element_type=jnp.float32) * HEAD_WIDTH ** (-0.5)
        scores = jnp.where(visible, scores, NEGATIVE)
        peak = lax.optimization_barrier(jnp.max(scores, -1, keepdims=True))
        weights = jnp.where(visible, jnp.exp(scores - peak), 0.0)
        denominator = lax.optimization_barrier(jnp.sum(weights, -1, keepdims=True))
        return jnp.dot(weights.astype(jnp.bfloat16), head_value, preferred_element_type=jnp.float32) / denominator
    attended = lax.map(attend_head, (queries_att.transpose(1, 0, 2), key_heads, value_heads))
    attention_out = (attended.transpose(1, 0, 2) * jax.nn.sigmoid(gating_att)).astype(jnp.bfloat16).reshape(SEQUENCE_LENGTH, QUERY_HEADS * HEAD_WIDTH)
    return (hidden_out, attention_out)
```

```python
import functools

import jax
import jax.numpy as jnp
from jax import lax
from jax.experimental import pallas as pl
from jax.experimental.pallas import tpu as pltpu
from jax.sharding import PartitionSpec as P

DK = 128
DV = 128
QUERY_HEADS = 16
KEY_VALUE_HEADS = 2
HEAD_WIDTH = 256
CONV = 4
EPSILON = 1e-06
NEGATIVE = -1e30
MESH = pl.DeviceIdType.MESH
BF = jnp.bfloat16
F32 = jnp.float32


def dot(a, b):
    return lax.dot_general(a, b, (((1,), (0,)), ((), ())), preferred_element_type=F32)


def dot_t(a, b):
    return lax.dot_general(a, b, (((1,), (1,)), ((), ())), preferred_element_type=F32)


def halves(a):
    high = a.astype(BF)
    return high, (a - high.astype(F32)).astype(BF)


def fine(a, b, mul=dot):
    ah, al = halves(a)
    bh, bl = halves(b)
    return mul(ah, bh) + (mul(ah, bl) + mul(al, bh))


def fine_left(a, b):
    ah, al = halves(a)
    return dot(ah, b) + dot(al, b)


def silu(x):
    return x / (1.0 + jnp.exp(-x))


def sigmoid(x):
    return 1.0 / (1.0 + jnp.exp(-x))


def softplus(x):
    u = jnp.exp(-jnp.abs(x))
    series = u * (1.0 - u * (0.5 - u * (1.0 / 3.0 - u * 0.25)))
    return jnp.maximum(x, 0.0) + jnp.where(u < 0.01, series, jnp.log(1.0 + u))


class Copy:
    def __init__(self, src, dst, send, recv, **where):
        self.copy = pltpu.make_async_remote_copy(
            src_ref=src, dst_ref=dst, send_sem=send, recv_sem=recv, device_id=where, device_id_type=MESH
        )

    def start(self):
        self.copy.start()

    def sent(self):
        self.copy.wait_send()

    def came(self):
        self.copy.wait_recv()


def kernel(
    NS,
    NH,
    residual,
    query_in,
    key_in,
    value_in,
    gating_in,
    beta_logit,
    decay_logit,
    seq_length,
    conv_query,
    conv_key,
    conv_value,
    decay_rate,
    norm_gain,
    out_weight,
    attn_gain,
    query_weight,
    key_value_weight,
    hidden_out,
    attention_out,
    qkv,
    halo,
    xp,
    gating,
    res,
    wout,
    wq,
    wkv,
    pair,
    in1,
    blk,
    in_r,
    in_l,
    pre,
    s_out,
    s_in,
    w_mat,
    u_mat,
    q_mat,
    a_mat,
    gated,
    part,
    pbuf,
    pin,
    hid,
    normed,
    kv,
    q_att,
    g_att,
    peak,
    total,
    accum,
    local,
    halo_s,
    halo_r,
    wq_s,
    wq_r,
    wkv_s,
    wkv_r,
    s1_s,
    s1_r,
    ag_s,
    ag_r,
    st_s,
    st_r,
    rs_s,
    rs_r,
    hg_s,
    hg_r,
    kr_s,
    kr_r,
    kl_s,
    kl_r,
    kx_s,
    kx_r,
):
    z = lax.axis_index("seq")
    h = lax.axis_index("head")
    rows = query_in.shape[0]
    kcols = query_in.shape[1]
    vcols = value_in.shape[1]
    heads = vcols // DV
    kheads = kcols // DK
    BLK = heads
    NB = NS // BLK
    b = z // BLK
    zl = z % BLK
    right = lax.rem(z + 1, NS)
    left = lax.rem(z + NS - 1, NS)
    far_r = lax.rem(z + BLK, NS)
    far_l = lax.rem(z + NS - BLK, NS)
    share = rows // NH
    core = h % 2
    other = h + 1 - 2 * core
    length = seq_length[0]
    wrows = query_weight.shape[0]

    barrier = pltpu.get_barrier_semaphore()

    def greet(**where):
        pl.semaphore_signal(barrier, inc=1, device_id=where, device_id_type=MESH)

    greet(seq=right)
    greet(seq=left)
    greet(seq=far_r)
    greet(seq=far_l)
    for d in range(1, BLK):
        greet(seq=b * BLK + lax.rem(zl + d, BLK))
    for d in range(1, NH):
        greet(head=lax.rem(h + d, NH))
    half = NS // 2
    early = half - 1

    @pl.when(z < early)
    def _():
        greet(seq=NS - 1)

    @pl.when(z == NS - 1)
    def _():
        for t in range(early):
            greet(seq=t)

    def fetch(i, src, dst):
        return pltpu.make_async_copy(src, dst, local.at[i])

    kvh = h // (NH // KEY_VALUE_HEADS)
    kv_start = pl.multiple_of((core * KEY_VALUE_HEADS + kvh) * HEAD_WIDTH, HEAD_WIDTH)
    fetches = [
        fetch(0, query_in, qkv.at[:, pl.ds(0, kcols)]),
        fetch(1, key_in, qkv.at[:, pl.ds(kcols, kcols)]),
        fetch(2, value_in, qkv.at[:, pl.ds(2 * kcols, vcols)]),
        fetch(3, query_weight, wq.at[pl.ds(pl.multiple_of(z * wrows, wrows), wrows)]),
        fetch(
            4,
            key_value_weight.at[:, pl.ds(kv_start, HEAD_WIDTH)],
            wkv.at[pl.ds(pl.multiple_of(z * wrows, wrows), wrows)],
        ),
        fetch(5, gating_in, gating),
        fetch(6, residual.at[pl.ds(pl.multiple_of(h * share, share), share)], res),
        fetch(7, out_weight, wout),
    ]
    for f in fetches:
        f.start()
    for f in fetches[:5]:
        f.wait()
    peers = 4 + (BLK - 1) + (NH - 1)
    pl.semaphore_wait(barrier, peers + jnp.where(z < early, 1, 0) + jnp.where(z == NS - 1, early, 0))

    halo_copy = Copy(qkv.at[pl.ds(rows - 16, 16)], halo, halo_s, halo_r, seq=right)
    halo_copy.start()

    steps_r, steps_l = NS // 2, (NS - 1) // 2

    def weight_copies(d, s):
        tile = lax.rem(z + NS - (s - 1), NS) if d == 0 else lax.rem(z + (s - 1), NS)
        at = pl.ds(pl.multiple_of(tile * wrows, wrows), wrows)
        to = right if d == 0 else left
        return (
            Copy(wkv.at[at], wkv.at[at], wkv_s.at[d, s - 1], wkv_r.at[d, s - 1], seq=to),
            Copy(wq.at[at], wq.at[at], wq_s.at[d, s - 1], wq_r.at[d, s - 1], seq=to),
        )

    def pump(s):
        for d, steps in ((0, steps_r), (1, steps_l)):
            if s > 1 and s - 1 <= steps:
                for c in weight_copies(d, s - 1):
                    c.came()
            if s <= steps:
                for c in weight_copies(d, s):
                    c.start()

    pump(1)

    halo_copy.came()
    tail = halo[...].astype(F32)[8:16]
    xp[0:8, :] = jnp.where(z > 0, tail, 0.0)
    xp[8 : 8 + rows, :] = qkv[...].astype(F32)

    def conv(taps, start, width):
        acc = jnp.zeros((rows, width), F32)
        for j in range(CONV):
            acc = acc + taps[j : j + 1, :] * xp[9 - CONV + j : 9 - CONV + j + rows, start : start + width]
        return silu(acc)

    def unit(x):
        return x * lax.rsqrt(jnp.sum(x * x, -1, keepdims=True) + EPSILON)

    qs = [unit(conv(conv_query[:, i * DK : (i + 1) * DK], i * DK, DK)) * DK**-0.5 for i in range(kheads)]
    ks = [unit(conv(conv_key[:, i * DK : (i + 1) * DK], kcols + i * DK, DK)) for i in range(kheads)]

    position = z * rows + lax.broadcasted_iota(jnp.int32, (rows, heads), 0)
    alive = (position < length).astype(F32)
    betas = sigmoid(beta_logit[...]) * alive
    log_decay = -decay_rate[...] * softplus(decay_logit[...]) * alive
    ri = lax.broadcasted_iota(jnp.int32, (rows, rows), 0)
    ci = lax.broadcasted_iota(jnp.int32, (rows, rows), 1)
    inclusive = ri >= ci
    strict = ri > ci
    tril = jnp.where(inclusive, 1.0, 0.0).astype(BF)
    pump(2)
    grams = [fine(k, k, dot_t) for k in ks]
    mixes = [fine(q, k, dot_t) for q, k in zip(qs, ks)]
    lowers, rights, kds, ends = [], [], [], []
    for v in range(heads):
        j = v * kheads // heads
        g = jnp.broadcast_to(log_decay[:, v : v + 1], (rows, rows))
        g1 = g.astype(BF)
        rest = g - g1.astype(F32)
        g2 = rest.astype(BF)
        g3 = (rest - g2.astype(F32)).astype(BF)
        run = dot(tril, g1) + (dot(tril, g2) + dot(tril, g3))
        spread = run - run.T
        within = jnp.where(inclusive, jnp.exp(jnp.where(inclusive, spread, 0.0)), 0.0)
        grow = jnp.exp(run)
        beta = betas[:, v : v + 1]
        lowers.append(jnp.where(strict, beta * within * grams[j], 0.0))
        value = conv(conv_value[:, v * DV : (v + 1) * DV], 2 * kcols + v * DV, DV)
        rights.append((beta * grow * ks[j], beta * value))
        end = run[rows - 1 : rows, :]
        kds.append((jnp.exp(end - run) * ks[j]).T)
        ends.append(jnp.exp(end))
        a_mat[v] = mixes[j] * within
        q_mat[v] = grow * qs[j]
    pump(3)
    eye = jnp.where(ri == ci, 1.0, 0.0)
    inverses = []
    for v in range(heads):
        inverses.append(eye - jnp.where((ri // 2 == ci // 2), lowers[v], 0.0))
    size = 2
    while size < rows:
        mask = (ri // (2 * size) == ci // (2 * size)) & (ri // size != ci // size)
        steps = [fine(jnp.where(mask, lowers[v], 0.0), inverses[v]) for v in range(heads)]
        inverses = [inverses[v] - fine(inverses[v], steps[v]) for v in range(heads)]
        size *= 2
    pump(4)
    for v in range(heads):
        solved = fine(inverses[v], jnp.concatenate(rights[v], 1))
        w_mat[v] = solved[:, :DK]
        u_mat[v] = solved[:, DK:]
        both = fine(kds[v], solved)
        pair[v, :, :DK] = (jnp.where(ri == ci, ends[v], 0.0) - both[:, :DK]).astype(BF)
        pair[v, :, DK:] = both[:, DK:].astype(BF)
    stage = []
    for d in range(1, BLK):
        to = lax.rem(zl + d, BLK)
        stage.append(Copy(pair.at[to], in1.at[zl], s1_s.at[d], s1_r.at[zl], seq=b * BLK + to))
        stage[-1].start()
    in1[zl] = pair[zl]
    pump(5)
    for d in range(1, BLK):
        frm = lax.rem(zl + d, BLK)
        Copy(in1.at[frm], in1.at[frm], s1_s.at[d], s1_r.at[frm], seq=right).came()
    running = in1[0].astype(F32)
    for i in range(1, BLK):
        pre[i] = running
        running = fine_right(in1[i][:, :DK], running)
        running = jnp.concatenate([running[:, :DK], running[:, DK:] + in1[i][:, DK:].astype(F32)], 1)
    blk[...] = running.astype(BF)
    ag_steps = (NB // 2, (NB - 1) // 2)
    CH = ag_s.shape[2]
    crow = DK // CH

    def ag_copy(d, s, k):
        at = pl.ds(k * crow, crow)
        buf = (in_r, in_l)[d]
        src = blk.at[at] if s == 1 else buf.at[s - 2, at]
        return Copy(
            src, buf.at[s - 1, at], ag_s.at[d, s - 1, k], ag_r.at[d, s - 1, k], seq=(far_r, far_l)[d]
        )

    for k in range(CH):
        for d in range(2):
            ag_copy(d, 1, k).start()
    pump(6)
    near_t = eye
    near_i = jnp.zeros((DK, DV), F32)
    far = jnp.zeros((DK, DV), F32)
    for s in range(1, ag_steps[0] + 1):
        for k in range(CH):
            for d in range(2):
                if s <= ag_steps[d]:
                    ag_copy(d, s, k).came()
                    if s + 1 <= ag_steps[d]:
                        ag_copy(d, s + 1, k).start()
        pump(6 + s)
        prod = fine_left(near_t, in_r[s - 1])
        ok = b - s >= 0
        near_i = jnp.where(ok, near_i + prod[:, DK:], near_i)
        near_t = jnp.where(ok, prod[:, :DK], near_t)
        if s <= ag_steps[1]:
            item = in_l[s - 1]
            nxt = fine_right(item[:, :DK], far) + item[:, DK:].astype(F32)
            far = jnp.where(b + s >= NB, nxt, far)
    entering = near_i + fine(near_t, far)
    done = 6 + ag_steps[0]
    s_out[0] = entering.astype(BF)
    for i in range(1, BLK):
        s_out[i] = (fine(pre[i][:, :DK], entering) + pre[i][:, DK:]).astype(BF)
    states = []
    for d in range(1, BLK):
        to = lax.rem(zl + d, BLK)
        states.append(Copy(s_out.at[to], s_in.at[zl], st_s.at[d], st_r.at[zl], seq=b * BLK + to))
        states[-1].start()
    s_in[zl] = s_out[zl]
    pump(done + 1)
    for d in range(1, BLK):
        frm = lax.rem(zl + d, BLK)
        Copy(s_in.at[frm], s_in.at[frm], st_s.at[d], st_r.at[frm], seq=right).came()

    for f in fetches[5:]:
        f.wait()
    for v in range(heads):
        lhs = jnp.concatenate([w_mat[v], q_mat[v]], 0)
        both = fine_left(lhs, s_in[v])
        delta = u_mat[v] - both[:rows]
        o = both[rows:] + fine(a_mat[v], delta)
        o = o * lax.rsqrt(jnp.mean(o * o, -1, keepdims=True) + EPSILON) * norm_gain[...]
        gate = silu(gating[:, v * DV : (v + 1) * DV].astype(F32))
        gated[:, v * DV : (v + 1) * DV] = (o * gate).astype(BF)
    width = wout.shape[1]
    strip = 512
    for n in range(0, width, strip):
        piece = dot(gated[...], wout[:, n : n + strip])
        part[:, n : n + strip] = piece
        pbuf[:, n : n + strip] = piece.astype(BF)
    mine = pl.ds(pl.multiple_of(h * share, share), share)

    def strip_of(i):
        return pl.ds(pl.multiple_of(i * share, share), share)

    sums = []
    for d in range(1, NH):
        to = lax.rem(h + d, NH)
        sums.append(Copy(pbuf.at[strip_of(to)], pin.at[h], rs_s.at[d], rs_r.at[h], head=to))
        sums[-1].start()
    pump(done + 2)
    acc = part[mine, :] + res[...].astype(F32)
    for d in range(1, NH):
        frm = lax.rem(h + d, NH)
        Copy(pin.at[frm], pin.at[frm], rs_s.at[d], rs_r.at[frm], head=frm).came()
        acc = acc + pin[frm].astype(F32)
    hid[mine, :] = acc.astype(BF)
    gathers = []
    for d in range(1, NH):
        to = lax.rem(h + d, NH)
        gathers.append(Copy(hid.at[mine], hid.at[mine], hg_s.at[d], hg_r.at[h], head=to))
        gathers[-1].start()
    pump(done + 3)
    for d in range(1, NH):
        frm = lax.rem(h + d, NH)
        Copy(hid.at[strip_of(frm)], hid.at[strip_of(frm)], hg_s.at[d], hg_r.at[frm], head=frm).came()
    save = pltpu.make_async_copy(hid, hidden_out, local.at[8])
    save.start()
    for n in range(0, rows, 32):
        x = hid[n : n + 32, :].astype(F32)
        x = x * lax.rsqrt(jnp.mean(x * x, -1, keepdims=True) + EPSILON) * attn_gain[...]
        normed[n : n + 32, :] = x.astype(BF)
    for s in range(done + 4, steps_r + 2):
        pump(s)

    kv[core, z] = dot(normed[...], wkv[...]).astype(BF)

    def kr_copy(s):
        item = z - (s - 1)
        return Copy(kv.at[core, item], kv.at[core, item], kr_s.at[s - 1], kr_r.at[s - 1], seq=right)

    def kl_copy(i):
        return Copy(kv.at[core, i], kv.at[core, i], kl_s.at[i], kl_r.at[i], seq=left)

    def kx_copy(i):
        return Copy(kv.at[core, i], kv.at[core, i], kx_s.at[i], kx_r.at[i], head=other)

    def kx_came(i):
        return Copy(kv.at[1 - core, i], kv.at[1 - core, i], kx_s.at[i], kx_r.at[i], head=other)

    @pl.when(z < NS - 1)
    def _():
        kr_copy(1).start()

    kx_copy(z).start()
    direct = Copy(kv.at[core, z], kv.at[core, z], kl_s.at[early], kl_r.at[z], seq=NS - 1)

    @pl.when(z < early)
    def _():
        direct.start()

    qrows = wq.shape[1] // (2 * HEAD_WIDTH)
    for i in range(qrows):
        at = 2 * i * HEAD_WIDTH
        q_att[i * rows : (i + 1) * rows, :] = (
            dot(normed[...], wq[:, at : at + HEAD_WIDTH]) * HEAD_WIDTH**-0.5
        ).astype(BF)
        g_att[i * rows : (i + 1) * rows, :] = dot(normed[...], wq[:, at + HEAD_WIDTH : at + 2 * HEAD_WIDTH])

    peak[...] = jnp.full(peak.shape, NEGATIVE, F32)
    total[...] = jnp.zeros(total.shape, F32)
    accum[...] = jnp.zeros(accum.shape, F32)

    def attend(item):
        scores = dot_t(q_att[...], kv[0, item])
        n = qrows * rows
        qpos = z * rows + lax.broadcasted_iota(jnp.int32, (n, rows), 0) % rows
        kpos = item * rows + lax.broadcasted_iota(jnp.int32, (n, rows), 1)
        visible = (kpos <= qpos) & (kpos < length)
        scores = jnp.where(visible, scores, NEGATIVE)
        old = peak[:, 0:1]
        new = jnp.maximum(old, jnp.max(scores, -1, keepdims=True))
        weights = jnp.where(visible, jnp.exp(scores - new), 0.0)
        scale = jnp.exp(old - new)
        peak[...] = jnp.broadcast_to(new, peak.shape)
        total[...] = total[...] * scale + jnp.sum(weights, -1, keepdims=True)
        accum[...] = accum[...] * scale + dot(weights.astype(BF), kv[1, item])

    kx_came(z).came()
    attend(z)

    @pl.loop(1, half + 1)
    def _(s):
        @pl.when(z - s >= 0)
        def _():
            item = z - s
            Copy(kv.at[core, item], kv.at[core, item], kr_s.at[s - 1], kr_r.at[s - 1], seq=right).came()

            @pl.when((s < half) & (z < NS - 1))
            def _():
                kr_copy(s + 1).start()

            kx_copy(item).start()

        i = s - 1

        @pl.when(i <= z - half - 1)
        def _():
            Copy(kv.at[core, i], kv.at[core, i], kl_s.at[i], kl_r.at[i], seq=left).came()

            @pl.when(i <= z - half - 2)
            def _():
                kl_copy(i).start()

            kx_copy(i).start()

        @pl.when(z - s >= 0)
        def _():
            kx_came(z - s).came()
            attend(z - s)

        @pl.when(i <= z - half - 1)
        def _():
            kx_came(i).came()
            attend(i)

    for i in range(qrows):
        at = slice(i * rows, (i + 1) * rows)
        o = accum[at, :] / total[at, 0:1] * sigmoid(g_att[at, :])
        attention_out[:, i * HEAD_WIDTH : (i + 1) * HEAD_WIDTH] = o.astype(BF)

    save.wait()
    halo_copy.sent()
    for d, steps in ((0, steps_r), (1, steps_l)):
        for s in range(1, steps + 1):
            for c in weight_copies(d, s):
                c.sent()
            for k in range(CH):
                if s <= ag_steps[d]:
                    ag_copy(d, s, k).sent()
    for c in stage + states + sums + gathers:
        c.sent()

    @pl.when(z < early)
    def _():
        direct.sent()

    @pl.loop(1, half + 1)
    def _(s):
        @pl.when((z - s + 1 >= 0) & (z < NS - 1))
        def _():
            kr_copy(s).sent()

        @pl.when(s - 1 <= z - half - 2)
        def _():
            kl_copy(s - 1).sent()

    @pl.loop(0, z + 1)
    def _(i):
        kx_copy(i).sent()


def fine_right(a, b):
    bh, bl = halves(b)
    return dot(a, bh) + dot(a, bl)


def shards(NS, NH, *args):
    (
        residual,
        query_in,
        key_in,
        value_in,
        gating_in,
        beta_logit,
        decay_logit,
        seq_length,
        conv_query,
        conv_key,
        conv_value,
        decay_rate,
        norm_gain,
        out_weight,
        attn_gain,
        query_weight,
        key_value_weight,
    ) = args
    rows, model = residual.shape
    kcols, vcols = query_in.shape[1], value_in.shape[1]
    heads = vcols // DV
    wcols = query_weight.shape[1]
    qheads = wcols // (2 * HEAD_WIDTH)
    nb = NS // heads
    half = NS // 2
    share = rows // NH
    ch = 4
    hbm = pl.BlockSpec(memory_space=pl.ANY)
    vmem = pl.BlockSpec(memory_space=pltpu.VMEM)
    smem = pl.BlockSpec(memory_space=pltpu.SMEM)
    dma = pltpu.SemaphoreType.DMA
    V = pltpu.VMEM
    scratch = [
        V((rows, 2 * kcols + vcols), BF),
        V((16, 2 * kcols + vcols), BF),
        V((rows + 8, 2 * kcols + vcols), F32),
        V((rows, vcols), BF),
        V((share, model), BF),
        V(out_weight.shape, BF),
        V((model, wcols), BF),
        V((model, HEAD_WIDTH), BF),
        V((heads, DK, DK + DV), BF),
        V((heads, DK, DK + DV), BF),
        V((DK, DK + DV), BF),
        V((nb // 2, DK, DK + DV), BF),
        V(((nb - 1) // 2, DK, DK + DV), BF),
        V((heads, DK, DK + DV), F32),
        V((heads, DK, DV), BF),
        V((heads, DK, DV), BF),
        V((heads, rows, DK), F32),
        V((heads, rows, DV), F32),
        V((heads, rows, DK), F32),
        V((heads, rows, rows), F32),
        V((rows, vcols), BF),
        V((rows, model), F32),
        V((rows, model), BF),
        V((NH, share, model), BF),
        V((rows, model), BF),
        V((rows, model), BF),
        V((2, NS, rows, HEAD_WIDTH), BF),
        V((qheads * rows, HEAD_WIDTH), BF),
        V((qheads * rows, HEAD_WIDTH), F32),
        V((qheads * rows, 128), F32),
        V((qheads * rows, 128), F32),
        V((qheads * rows, HEAD_WIDTH), F32),
        dma((9,)),
        dma,
        dma,
        dma((2, half)),
        dma((2, half)),
        dma((2, half)),
        dma((2, half)),
        dma((heads,)),
        dma((heads,)),
        dma((2, nb // 2, ch)),
        dma((2, nb // 2, ch)),
        dma((heads,)),
        dma((heads,)),
        dma((NH,)),
        dma((NH,)),
        dma((NH,)),
        dma((NH,)),
        dma((half,)),
        dma((half,)),
        dma((half,)),
        dma((half,)),
        dma((NS,)),
        dma((NS,)),
    ]
    return pl.pallas_call(
        functools.partial(kernel, NS, NH),
        name="layer",
        out_shape=(
            jax.ShapeDtypeStruct((rows, model), BF),
            jax.ShapeDtypeStruct((rows, qheads * HEAD_WIDTH), BF),
        ),
        in_specs=[hbm, hbm, hbm, hbm, hbm, vmem, vmem, smem, vmem, vmem, vmem, vmem, vmem, hbm, vmem, hbm, hbm],
        out_specs=(hbm, vmem),
        scratch_shapes=scratch,
        compiler_params=pltpu.CompilerParams(
            collective_id=0, has_side_effects=True, vmem_limit_bytes=56 * 1024 * 1024
        ),
    )(
        residual,
        query_in,
        key_in,
        value_in,
        gating_in,
        beta_logit,
        decay_logit,
        seq_length,
        conv_query,
        conv_key,
        conv_value,
        decay_rate.reshape(1, -1),
        norm_gain.reshape(1, -1),
        out_weight,
        attn_gain.reshape(1, -1),
        query_weight,
        key_value_weight,
    )


def solution(mesh):
    placed = (
        P(("groups", "seq"), None),
        P(("groups", "seq"), "head"),
        P(("groups", "seq"), "head"),
        P(("groups", "seq"), "head"),
        P(("groups", "seq"), "head"),
        P(("groups", "seq"), "head"),
        P(("groups", "seq"), "head"),
        P("groups"),
        P(None, "head"),
        P(None, "head"),
        P(None, "head"),
        P("head"),
        P(),
        P("head", None),
        P(),
        P("seq", "head"),
        P("seq", None),
    )
    return jax.shard_map(
        functools.partial(shards, mesh.shape["seq"], mesh.shape["head"]),
        mesh=mesh,
        in_specs=placed,
        out_specs=(P(("groups", "seq"), None), P(("groups", "seq"), "head")),
        check_vma=False,
    )
```

```python
import functools

import jax
import jax.numpy as jnp
from jax import lax
from jax.experimental import pallas as pl
from jax.experimental.pallas import tpu as pltpu
from jax.sharding import PartitionSpec as P

DK = 128
DV = 128
QUERY_HEADS = 16
KEY_VALUE_HEADS = 2
HEAD_WIDTH = 256
CONV = 4
PART = HEAD_WIDTH // 2
EPSILON = 1e-06
NEGATIVE = -1e30
MESH = pl.DeviceIdType.MESH
BF = jnp.bfloat16
F32 = jnp.float32


def dot(a, b):
    return lax.dot_general(a, b, (((1,), (0,)), ((), ())), preferred_element_type=F32)


def dot_t(a, b):
    return lax.dot_general(a, b, (((1,), (1,)), ((), ())), preferred_element_type=F32)


def halves(a):
    high = a.astype(BF)
    return high, (a - high.astype(F32)).astype(BF)


def fine(a, b, mul=dot):
    ah, al = halves(a)
    bh, bl = halves(b)
    return mul(ah, bh) + (mul(ah, bl) + mul(al, bh))


def fine_left(a, b):
    ah, al = halves(a)
    return dot(ah, b) + dot(al, b)


def silu(x):
    return x / (1.0 + jnp.exp(-x))


def sigmoid(x):
    return 1.0 / (1.0 + jnp.exp(-x))


def softplus(x):
    u = jnp.exp(-jnp.abs(x))
    series = u * (1.0 - u * (0.5 - u * (1.0 / 3.0 - u * 0.25)))
    return jnp.maximum(x, 0.0) + jnp.where(u < 0.01, series, jnp.log(1.0 + u))


class Copy:
    def __init__(self, src, dst, send, recv, **where):
        self.copy = pltpu.make_async_remote_copy(
            src_ref=src, dst_ref=dst, send_sem=send, recv_sem=recv, device_id=where, device_id_type=MESH
        )

    def start(self):
        self.copy.start()

    def sent(self):
        self.copy.wait_send()

    def came(self):
        self.copy.wait_recv()


def kernel(
    NG,
    NS,
    NH,
    residual,
    query_in,
    key_in,
    value_in,
    gating_in,
    beta_logit,
    decay_logit,
    seq_length,
    conv_query,
    conv_key,
    conv_value,
    decay_rate,
    norm_gain,
    out_weight,
    attn_gain,
    query_weight,
    key_value_weight,
    hidden_out,
    attention_out,
    qkv,
    halo,
    xp,
    gating,
    res,
    wout,
    wq,
    wkv,
    pair,
    in1,
    blk,
    in_r,
    in_l,
    pre,
    near,
    distant,
    s_out,
    s_in,
    w_mat,
    u_mat,
    q_mat,
    a_mat,
    gated,
    part,
    pbuf,
    pin,
    hid,
    normed,
    kv,
    q_att,
    g_att,
    peak,
    total,
    accum,
    local,
    halo_s,
    halo_r,
    wq_s,
    wq_r,
    wkv_s,
    wkv_r,
    wy_s,
    wy_r,
    s1_s,
    s1_r,
    ag_s,
    ag_r,
    st_s,
    st_r,
    rs_s,
    rs_r,
    hg_s,
    hg_r,
    kr_s,
    kr_r,
    kl_s,
    kl_r,
    kx_s,
    kx_r,
    from_left,
    from_right,
    row_in,
    row_known,
    last_known,
):
    z = lax.axis_index("seq")
    h = lax.axis_index("head")
    g = lax.axis_index("groups")
    rows = query_in.shape[0]
    kcols = query_in.shape[1]
    vcols = value_in.shape[1]
    heads = vcols // DV
    kheads = kcols // DK
    BLK = heads
    NB = NS // BLK
    b = z // BLK
    zl = z % BLK
    right = lax.rem(z + 1, NS)
    left = lax.rem(z + NS - 1, NS)
    far_r = lax.rem(z + BLK, NS)
    far_l = lax.rem(z + NS - BLK, NS)
    share = rows // NH
    core = h % 2
    other = h + 1 - 2 * core
    side = (h // 2) % 2
    across = h + 2 - 4 * side
    mine_q, twin_q = 2 * side + core, 2 * side + 1 - core
    across_q, last_q = 2 * (1 - side) + core, 2 * (1 - side) + 1 - core
    paired = NG % 2 == 0
    turn = g % 2 if paired else 0
    ally = g + 1 - 2 * turn
    length = seq_length[0]
    wrows = query_weight.shape[0]

    barrier = pltpu.get_barrier_semaphore()

    def greet(**where):
        pl.semaphore_signal(barrier, inc=1, device_id=where, device_id_type=MESH)

    hop_r = lax.rem(z + 2, NS)
    hop_l = lax.rem(z + NS - 2, NS)
    for to in (right, left, hop_r, hop_l):
        greet(seq=to)
    if paired:
        greet(groups=ally)
    odd = z % 2 == 1

    @pl.when(odd)
    def _():
        for d in range(1, NH):
            greet(head=lax.rem(h + d, NH))

    half = NS // 2
    early = half - 1
    wrapped = (NB - 1) // 2

    def fetch(i, src, dst):
        return pltpu.make_async_copy(src, dst, local.at[i])

    kvh = h // (NH // KEY_VALUE_HEADS)
    kv_start = pl.multiple_of((side * KEY_VALUE_HEADS + kvh) * HEAD_WIDTH + core * PART, PART)
    fetches = [
        fetch(0, query_in, qkv.at[:, pl.ds(0, kcols)]),
        fetch(1, key_in, qkv.at[:, pl.ds(kcols, kcols)]),
        fetch(2, value_in, qkv.at[:, pl.ds(2 * kcols, vcols)]),
        fetch(3, query_weight, wq.at[pl.ds(pl.multiple_of(z * wrows, wrows), wrows)]),
        fetch(
            4,
            key_value_weight.at[:, pl.ds(kv_start, PART)],
            wkv.at[pl.ds(pl.multiple_of(z * wrows, wrows), wrows)],
        ),
        fetch(5, gating_in, gating),
        fetch(6, residual.at[pl.ds(pl.multiple_of(h * share, share), share)], res),
        fetch(7, out_weight, wout),
    ]
    for f in fetches:
        f.start()
    for f in fetches[:5]:
        f.wait()
    pl.semaphore_wait(barrier, 4 + (1 if paired else 0) + jnp.where(odd, NH - 1, 0))

    def tell(sem, **where):
        pl.semaphore_signal(sem, inc=1, device_id=where, device_id_type=MESH)

    tell(from_left, seq=hop_r)
    tell(from_right, seq=hop_l)

    @pl.when(odd)
    def _():
        for d in range(1, NH):
            tell(row_in, head=lax.rem(h + d, NH))

    halo_copy = Copy(qkv.at[pl.ds(rows - 16, 16)], halo, halo_s, halo_r, seq=right)
    halo_copy.start()

    steps_r, steps_l = NS // 2, (NS - 1) // 2
    owners = 2 if paired else 1
    wide = wq.shape[1] // (2 * owners)

    def columns(stream, owner):
        return pl.ds(pl.multiple_of((owner * 2 + stream) * wide, wide), wide)

    def tile_rows(tile):
        return pl.ds(pl.multiple_of(tile * wrows, wrows), wrows)

    def tile_at(d, distance):
        return lax.rem(z + NS - distance, NS) if d == 0 else lax.rem(z + distance, NS)

    def weight_copies(stream, d, distance, hops):
        at = tile_rows(tile_at(d, distance))
        to = ((right, left), (hop_r, hop_l))[hops - 1][d]
        sem = distance + hops - 1
        refs = [(wq.at[at, columns(stream, turn)], wq_s.at[stream, d, sem], wq_r.at[stream, d, sem])]
        if stream == 0:
            refs.insert(0, (wkv.at[at], wkv_s.at[d, sem], wkv_r.at[d, sem]))
        return [Copy(ref, ref, send, recv, seq=to) for ref, send, recv in refs]

    def weight_came(stream, d, distance):
        at = tile_rows(tile_at(d, distance))
        sem = distance - 1
        if stream == 0:
            Copy(wkv.at[at], wkv.at[at], wkv_s.at[d, sem], wkv_r.at[d, sem], seq=right).came()
        ref = wq.at[at, columns(stream, turn)]
        Copy(ref, ref, wq_s.at[stream, d, sem], wq_r.at[stream, d, sem], seq=right).came()

    reach = (steps_r, steps_l)

    def weight_sends(stream, d, k):
        return [
            c for hops in (2, 1) if 2 * k + hops <= reach[d] for c in weight_copies(stream, d, 2 * k, hops)
        ]

    def ally_copy(stream, tile, owner=None):
        ref = wq.at[tile_rows(tile), columns(stream, turn if owner is None else owner)]
        return Copy(ref, ref, wy_s.at[stream, tile], wy_r.at[stream, tile], groups=ally)

    turns = [(stream, k) for k in range(NS // 4 + 1) for stream in range(2)]

    def pump(count):
        for stream, k in turns[:count]:
            for d in range(2):
                if 0 < 2 * k <= reach[d]:
                    weight_came(stream, d, 2 * k)
                for c in weight_sends(stream, d, k):
                    c.start()
            for d in range(2):
                if 0 < 2 * k - 1 <= reach[d]:
                    weight_came(stream, d, 2 * k - 1)
            for d in range(2):
                for distance in (2 * k - 1, 2 * k):
                    if 0 < distance <= reach[d] and paired:
                        ally_copy(stream, tile_at(d, distance)).start()
        del turns[:count]

    pump(2)

    @pl.when(z > 0)
    def _():
        halo_copy.came()
        xp[0:8, :] = halo[...].astype(F32)[8:16]

    @pl.when(z == 0)
    def _():
        xp[0:8, :] = jnp.zeros((8, xp.shape[1]), F32)

    xp[8 : 8 + rows, :] = qkv[...].astype(F32)

    def conv(taps, start, width):
        acc = jnp.zeros((rows, width), F32)
        for j in range(CONV):
            acc = acc + taps[j : j + 1, :] * xp[9 - CONV + j : 9 - CONV + j + rows, start : start + width]
        return silu(acc)

    def unit(x):
        return x * lax.rsqrt(jnp.sum(x * x, -1, keepdims=True) + EPSILON)

    qs = [unit(conv(conv_query[:, i * DK : (i + 1) * DK], i * DK, DK)) * DK**-0.5 for i in range(kheads)]
    ks = [unit(conv(conv_key[:, i * DK : (i + 1) * DK], kcols + i * DK, DK)) for i in range(kheads)]

    position = z * rows + lax.broadcasted_iota(jnp.int32, (heads, rows), 1)
    alive = (position < length).astype(F32)
    betas = sigmoid(beta_logit[...]) * alive
    log_decay = -decay_rate[...] * softplus(decay_logit[...]) * alive
    ri = lax.broadcasted_iota(jnp.int32, (rows, rows), 0)
    ci = lax.broadcasted_iota(jnp.int32, (rows, rows), 1)
    inclusive = ri >= ci
    strict = ri > ci
    triu = jnp.where(ri <= ci, 1.0, 0.0).astype(BF)
    g1 = log_decay.astype(BF)
    rest = log_decay - g1.astype(F32)
    g2 = rest.astype(BF)
    g3 = (rest - g2.astype(F32)).astype(BF)
    runs = dot(g1, triu) + (dot(g2, triu) + dot(g3, triu))
    grams = [fine(k, k, dot_t) for k in ks]
    mixes = [fine(q, k, dot_t) for q, k in zip(qs, ks)]
    lowers, rights, kds, ends = [], [], [], []
    for v in range(heads):
        j = v * kheads // heads
        row = jnp.broadcast_to(runs[v : v + 1, :], (rows, rows))
        run = row.T
        spread = run - row
        within = jnp.where(inclusive, jnp.exp(jnp.where(inclusive, spread, 0.0)), 0.0)
        grow = jnp.exp(run)
        beta = jnp.broadcast_to(betas[v : v + 1, :], (rows, rows)).T
        lowers.append(jnp.where(strict, beta * within * grams[j], 0.0))
        value = conv(conv_value[:, v * DV : (v + 1) * DV], 2 * kcols + v * DV, DV)
        rights.append((beta * grow * ks[j], beta * value))
        end = run[rows - 1 : rows, :]
        kds.append((jnp.exp(end - run) * ks[j]).T)
        ends.append(jnp.exp(end))
        a_mat[v] = mixes[j] * within
        q_mat[v] = grow * qs[j]
    eye = jnp.where(ri == ci, 1.0, 0.0)
    inverses = []
    for v in range(heads):
        inverses.append(eye - jnp.where((ri // 2 == ci // 2), lowers[v], 0.0))
    size = 2
    while size < rows:
        mask = (ri // (2 * size) == ci // (2 * size)) & (ri // size != ci // size)
        steps = [fine(jnp.where(mask, lowers[v], 0.0), inverses[v]) for v in range(heads)]
        inverses = [inverses[v] - fine(inverses[v], steps[v]) for v in range(heads)]
        size *= 2
    for v in range(heads):
        solved = fine(inverses[v], jnp.concatenate(rights[v], 1))
        w_mat[v] = solved[:, :DK]
        u_mat[v] = solved[:, DK:]
        both = fine(kds[v], solved)
        pair[v, :, :DK] = (jnp.where(ri == ci, ends[v], 0.0) - both[:, :DK]).astype(BF)
        pair[v, :, DK:] = both[:, DK:].astype(BF)
    pl.semaphore_wait(from_right, 1)
    last_in_block = zl == BLK - 1

    @pl.when(last_in_block)
    def _():
        pl.semaphore_wait(from_left, 1)

    stage = []
    for d in range(1, BLK):
        to = lax.rem(zl + d, BLK)
        stage.append(Copy(pair.at[to], in1.at[zl], s1_s.at[d], s1_r.at[zl], seq=b * BLK + to))
        stage[-1].start()
    in1[zl] = pair[zl]
    pump(2)
    for d in range(1, BLK):
        frm = lax.rem(zl + d, BLK)
        Copy(in1.at[frm], in1.at[frm], s1_s.at[d], s1_r.at[frm], seq=right).came()
    running = in1[0].astype(F32)
    for i in range(1, BLK):
        pre[i] = running
        running = fine_right(in1[i][:, :DK], running)
        running = jnp.concatenate([running[:, :DK], running[:, DK:] + in1[i][:, DK:].astype(F32)], 1)
    blk[...] = running.astype(BF)
    ahead = NB // 2
    CH = ag_s.shape[2]
    crow = DK // CH

    def ag_copy(buf, src, d, slot, k, to):
        at = pl.ds(k * crow, crow)
        return Copy(src.at[at], buf.at[slot, at], ag_s.at[d, slot, k], ag_r.at[d, slot, k], seq=to)

    def ag_right(s, k):
        return ag_copy(in_r, blk if s == 1 else in_r.at[s - 2], 0, s - 1, k, far_r)

    def ag_left(s, k):
        return ag_copy(in_l, blk if s == 1 else in_l.at[s - 2], 1, s - 1, k, far_l)

    def goes_right(s):
        return (b >= s - 1) & (b < NB - 1)

    def left_at(place, s):
        return (place + s >= NB) | (place + s < wrapped)

    def goes_left(s):
        return left_at(lax.rem(b + NB - 1, NB), s)

    @pl.when(goes_right(1))
    def _():
        for k in range(CH):
            ag_right(1, k).start()

    @pl.when(jnp.logical_not(last_in_block))
    def _():
        pl.semaphore_wait(from_left, 1)

    @pl.when(goes_left(1))
    def _():
        for k in range(CH):
            ag_left(1, k).start()

    pump(2)
    eye2 = jnp.concatenate([eye, jnp.zeros((DK, DV), F32)], 1)
    near[...] = eye2
    distant[...] = jnp.zeros((DK, DV), F32)
    for s in range(1, ahead + 1):

        @pl.when(b >= s)
        def _(s=s):
            for k in range(CH):
                ag_right(s, k).came()
                if s < ahead:

                    @pl.when(goes_right(s + 1))
                    def _(k=k):
                        ag_right(s + 1, k).start()

        if s <= wrapped:

            @pl.when(left_at(b, s))
            def _(s=s):
                for k in range(CH):
                    ag_left(s, k).came()
                    if s < wrapped:

                        @pl.when(goes_left(s + 1))
                        def _(k=k):
                            ag_left(s + 1, k).start()

        pump(2)

        @pl.when(b >= s)
        def _(s=s):
            item = in_r[s - 1]
            if s == 1:
                near[...] = item.astype(F32)
            else:
                prod = fine_left(near[:, :DK], item)
                near[:, DK:] = near[:, DK:] + prod[:, DK:]
                near[:, :DK] = prod[:, :DK]

        if s <= wrapped:

            @pl.when(b + s >= NB)
            def _(s=s):
                item = in_l[s - 1]
                distant[...] = fine_right(item[:, :DK], distant[...]) + item[:, DK:].astype(F32)

    entering = near[:, DK:] + fine(near[:, :DK], distant[...])

    @pl.when(odd)
    def _():
        pl.semaphore_wait(row_in, NH - 1)
        tell(row_known, seq=left)

    @pl.when((z > 0) & (z < early))
    def _():
        pl.semaphore_wait(last_known, 1)

    @pl.when(z < early - 1)
    def _():
        tell(last_known, seq=right)

    s_out[0] = entering.astype(BF)
    for i in range(1, BLK):
        s_out[i] = (fine(pre[i][:, :DK], entering) + pre[i][:, DK:]).astype(BF)
    states = []
    for d in range(1, BLK):
        to = lax.rem(zl + d, BLK)
        states.append(Copy(s_out.at[to], s_in.at[zl], st_s.at[d], st_r.at[zl], seq=b * BLK + to))
        states[-1].start()
    s_in[zl] = s_out[zl]
    pump(1)
    for d in range(1, BLK):
        frm = lax.rem(zl + d, BLK)
        Copy(s_in.at[frm], s_in.at[frm], st_s.at[d], st_r.at[frm], seq=right).came()

    for f in fetches[5:]:
        f.wait()
    for v in range(heads):
        lhs = jnp.concatenate([w_mat[v], q_mat[v]], 0)
        both = fine_left(lhs, s_in[v])
        delta = u_mat[v] - both[:rows]
        o = both[rows:] + fine(a_mat[v], delta)
        o = o * lax.rsqrt(jnp.mean(o * o, -1, keepdims=True) + EPSILON) * norm_gain[...]
        gate = silu(gating[:, v * DV : (v + 1) * DV].astype(F32))
        gated[:, v * DV : (v + 1) * DV] = (o * gate).astype(BF)
    width = wout.shape[1]
    strip = 512
    for n in range(0, width, strip):
        piece = dot(gated[...], wout[:, n : n + strip])
        part[:, n : n + strip] = piece
        pbuf[:, n : n + strip] = piece.astype(BF)
    mine = pl.ds(pl.multiple_of(h * share, share), share)

    def strip_of(i):
        return pl.ds(pl.multiple_of(i * share, share), share)

    @pl.when(jnp.logical_not(odd))
    def _():
        pl.semaphore_wait(row_known, 1)

    sums = []
    for d in range(1, NH):
        to = lax.rem(h + d, NH)
        sums.append(Copy(pbuf.at[strip_of(to)], pin.at[h], rs_s.at[d], rs_r.at[h], head=to))
        sums[-1].start()
    pump(1)
    acc = part[mine, :] + res[...].astype(F32)
    for d in range(1, NH):
        frm = lax.rem(h + d, NH)
        Copy(pin.at[frm], pin.at[frm], rs_s.at[d], rs_r.at[frm], head=frm).came()
        acc = acc + pin[frm].astype(F32)
    hid[mine, :] = acc.astype(BF)
    gathers = []
    for d in range(1, NH):
        to = lax.rem(h + d, NH)
        gathers.append(Copy(hid.at[mine], hid.at[mine], hg_s.at[d], hg_r.at[h], head=to))
        gathers[-1].start()
    pump(2)
    for d in range(1, NH):
        frm = lax.rem(h + d, NH)
        Copy(hid.at[strip_of(frm)], hid.at[strip_of(frm)], hg_s.at[d], hg_r.at[frm], head=frm).came()
    save = pltpu.make_async_copy(hid, hidden_out, local.at[8])
    save.start()
    for n in range(0, rows, 32):
        x = hid[n : n + 32, :].astype(F32)
        x = x * lax.rsqrt(jnp.mean(x * x, -1, keepdims=True) + EPSILON) * attn_gain[...]
        normed[n : n + 32, :] = x.astype(BF)
    pump(len(turns))

    kv[mine_q, z] = dot(normed[...], wkv[...]).astype(BF)

    def item_copy(i, sends, recvs, at_send, at_recv, **where):
        return Copy(kv.at[mine_q, i], kv.at[mine_q, i], sends.at[at_send], recvs.at[at_recv], **where)

    def kr_near(k):
        return item_copy(z - 2 * k, kr_s, kr_r, 2 * k, 2 * k, seq=right)

    def kr_far(k):
        return item_copy(z - 2 * k, kr_s, kr_r, 2 * k + 1, 2 * k + 1, seq=hop_r)

    def kr_sends(k):
        have = (z >= 2 * k) & (2 * k < half)
        return have & (z < NS - 2), have & (z < NS - 1)

    def kl_near(i):
        return item_copy(i, kl_s, kl_r, 2 * i, i, seq=left)

    def kl_far(i):
        return item_copy(i, kl_s, kl_r, 2 * i + 1, i, seq=hop_l)

    def kl_has(i):
        return i <= z - half - 1

    def kl_sends(i):
        passes = (NS - 1 - z) % 2 == 0
        return passes & (i <= z - half - 3), passes & (i <= z - half - 2)

    def share_copy(lane, quarter, i, head):
        return Copy(kv.at[quarter, i], kv.at[quarter, i], kx_s.at[lane, i], kx_r.at[lane, i], head=head)

    def share(i):
        share_copy(1, mine_q, i, across).start()
        share_copy(0, mine_q, i, other).start()

    def relay(i):
        share_copy(1, across_q, i, across).came()
        share_copy(2, across_q, i, other).start()

    def gather(i):
        share_copy(0, twin_q, i, other).came()
        share_copy(2, last_q, i, other).came()

    def start_if(conditions, copies):
        for condition, copy in zip(conditions, copies):

            @pl.when(condition)
            def _(copy=copy):
                copy.start()

    start_if(kr_sends(0), (kr_far(0), kr_near(0)))
    direct = item_copy(z, kl_s, kl_r, 2 * early, z, seq=NS - 1)
    start_if((z < early,), (direct,))
    share(z)

    if paired:

        @pl.loop(1, NS)
        def _(d):
            for stream in range(2):
                ally_copy(stream, lax.rem(z + d, NS), 1 - turn).came()

    qrows = wq.shape[1] // (2 * HEAD_WIDTH)
    for i in range(qrows):
        at = 2 * i * HEAD_WIDTH
        q_att[i * rows : (i + 1) * rows, :] = (
            dot(normed[...], wq[:, at : at + HEAD_WIDTH]) * HEAD_WIDTH**-0.5
        ).astype(BF)
        g_att[i * rows : (i + 1) * rows, :] = dot(normed[...], wq[:, at + HEAD_WIDTH : at + 2 * HEAD_WIDTH])

    peak[...] = jnp.full(peak.shape, NEGATIVE, F32)
    total[...] = jnp.zeros(total.shape, F32)
    accum[...] = jnp.zeros(accum.shape, F32)

    def attend(items, own=False):
        parts = []
        for item in items:
            scores = dot_t(q_att[:, :PART], kv[0, item]) + dot_t(q_att[:, PART:], kv[1, item])
            n = qrows * rows if own else 1
            kpos = item * rows + lax.broadcasted_iota(jnp.int32, (n, rows), 1)
            visible = kpos < length
            if own:
                qpos = z * rows + lax.broadcasted_iota(jnp.int32, (n, rows), 0) % rows
                visible = visible & (kpos <= qpos)
            parts.append((item, jnp.where(visible, scores, NEGATIVE), visible))
        top = functools.reduce(jnp.maximum, [scores for _, scores, _ in parts])
        old = peak[...]
        new = jnp.maximum(old, jnp.max(top, -1, keepdims=True))
        scale = jnp.exp(old - new)
        peak[...] = new
        weights = [(item, jnp.where(visible, jnp.exp(scores - new), 0.0)) for item, scores, visible in parts]
        sums = functools.reduce(jnp.add, [w for _, w in weights])
        total[...] = total[...] * scale + jnp.sum(sums, -1, keepdims=True)
        weights = [(item, w.astype(BF)) for item, w in weights]
        for i in range(2):
            at = slice(i * PART, (i + 1) * PART)
            more = functools.reduce(jnp.add, [dot(w, kv[2 + i, item]) for item, w in weights])
            accum[:, at] = accum[:, at] * scale + more

    rounds = half // 2

    def items_of(k):
        near, far = z - (2 * k - 1), z - 2 * k
        turn_l = k - (NS - z) // 2
        i, j = 2 * turn_l - 2, 2 * turn_l - 1
        comes = turn_l >= 1
        return (near, near >= 0), (far, far >= 0), (i, comes & kl_has(i)), (j, comes & kl_has(j) & (j < early))

    def take(k):
        (near, has_near), (far, has_far), (i, has_i), (j, has_j) = items_of(k)
        for items, condition in (
            ((near, far, i, j), has_far & has_j),
            ((near, far), has_far & jnp.logical_not(has_j)),
            ((near,), has_near & jnp.logical_not(has_far)),
            ((i, j), has_j & jnp.logical_not(has_far)),
            ((i,), has_i & jnp.logical_not(has_j)),
        ):

            @pl.when(condition)
            def _(items=items):
                for item in items:
                    gather(item)
                attend(items)

    def pass_on(k):
        for item, condition in items_of(k):

            @pl.when(condition)
            def _(item=item):
                relay(item)

    @pl.loop(1, rounds + 3)
    def _(k):
        (near, has_near), (far, has_far), (i, has_i), (j, has_j) = items_of(k)

        @pl.when(has_far & (k <= rounds))
        def _():
            item_copy(far, kr_s, kr_r, 2 * k - 1, 2 * k - 1, seq=right).came()
            start_if(kr_sends(k), (kr_far(k), kr_near(k)))
            share(far)

        @pl.when(has_near & (k <= rounds))
        def _():
            item_copy(near, kr_s, kr_r, 2 * k - 2, 2 * k - 2, seq=right).came()
            share(near)

        for item, condition in ((i, has_i), (j, has_j)):

            @pl.when(condition & (k <= rounds))
            def _(item=item):
                item_copy(item, kl_s, kl_r, 2 * item, item, seq=left).came()
                start_if(kl_sends(item), (kl_far(item), kl_near(item)))
                share(item)

        @pl.when(k == 1)
        def _():
            relay(z)

        @pl.when((k > 1) & (k <= rounds + 1))
        def _():
            pass_on(k - 1)

        @pl.when(k == 2)
        def _():
            gather(z)
            attend((z,), own=True)

        @pl.when(k > 2)
        def _():
            take(k - 2)

    for i in range(qrows):
        at = slice(i * rows, (i + 1) * rows)
        o = accum[at, :] / total[at, 0:1] * sigmoid(g_att[at, :])
        attention_out[:, i * HEAD_WIDTH : (i + 1) * HEAD_WIDTH] = o.astype(BF)

    save.wait()
    halo_copy.sent()

    @pl.when(z == 0)
    def _():
        halo_copy.came()

    for d in range(2):
        for stream in range(2):
            for k in range(NS // 4):
                for c in weight_sends(stream, d, k):
                    c.sent()
    for c in stage + states + sums + gathers:
        c.sent()
    for s in range(1, ahead + 1):

        @pl.when(goes_right(s))
        def _(s=s):
            for k in range(CH):
                ag_right(s, k).sent()

    for s in range(1, wrapped + 1):

        @pl.when(goes_left(s))
        def _(s=s):
            for k in range(CH):
                ag_left(s, k).sent()


    def sent_if(conditions, copies):
        for condition, copy in zip(conditions, copies):

            @pl.when(condition)
            def _(copy=copy):
                copy.sent()

    sent_if((z < early,), (direct,))

    @pl.loop(0, rounds)
    def _(k):
        sent_if(kr_sends(k), (kr_far(k), kr_near(k)))

    @pl.loop(0, early)
    def _(i):
        sent_if(kl_sends(i), (kl_far(i), kl_near(i)))

    @pl.loop(0, z + 1)
    def _(i):
        for lane, quarter, to in ((0, mine_q, other), (1, mine_q, across), (2, across_q, other)):
            share_copy(lane, quarter, i, to).sent()

    if paired:

        @pl.loop(1, NS)
        def _(d):
            for stream in range(2):
                ally_copy(stream, lax.rem(z + d, NS)).sent()


def fine_right(a, b):
    bh, bl = halves(b)
    return dot(a, bh) + dot(a, bl)


def shards(NG, NS, NH, *args):
    (
        residual,
        query_in,
        key_in,
        value_in,
        gating_in,
        beta_logit,
        decay_logit,
        seq_length,
        conv_query,
        conv_key,
        conv_value,
        decay_rate,
        norm_gain,
        out_weight,
        attn_gain,
        query_weight,
        key_value_weight,
    ) = args
    rows, model = residual.shape
    kcols, vcols = query_in.shape[1], value_in.shape[1]
    heads = vcols // DV
    wcols = query_weight.shape[1]
    qheads = wcols // (2 * HEAD_WIDTH)
    nb = NS // heads
    half = NS // 2
    share = rows // NH
    ch = 4
    hbm = pl.BlockSpec(memory_space=pl.ANY)
    vmem = pl.BlockSpec(memory_space=pltpu.VMEM)
    smem = pl.BlockSpec(memory_space=pltpu.SMEM)
    dma = pltpu.SemaphoreType.DMA
    V = pltpu.VMEM
    scratch = [
        V((rows, 2 * kcols + vcols), BF),
        V((16, 2 * kcols + vcols), BF),
        V((rows + 8, 2 * kcols + vcols), F32),
        V((rows, vcols), BF),
        V((share, model), BF),
        V(out_weight.shape, BF),
        V((model, wcols), BF),
        V((model, PART), BF),
        V((heads, DK, DK + DV), BF),
        V((heads, DK, DK + DV), BF),
        V((DK, DK + DV), BF),
        V((nb // 2, DK, DK + DV), BF),
        V(((nb - 1) // 2, DK, DK + DV), BF),
        V((heads, DK, DK + DV), F32),
        V((DK, DK + DV), F32),
        V((DK, DV), F32),
        V((heads, DK, DV), BF),
        V((heads, DK, DV), BF),
        V((heads, rows, DK), F32),
        V((heads, rows, DV), F32),
        V((heads, rows, DK), F32),
        V((heads, rows, rows), F32),
        V((rows, vcols), BF),
        V((rows, model), F32),
        V((rows, model), BF),
        V((NH, share, model), BF),
        V((rows, model), BF),
        V((rows, model), BF),
        V((4, NS, rows, PART), BF),
        V((qheads * rows, HEAD_WIDTH), BF),
        V((qheads * rows, HEAD_WIDTH), F32),
        V((qheads * rows, 128), F32),
        V((qheads * rows, 128), F32),
        V((qheads * rows, HEAD_WIDTH), F32),
        dma((9,)),
        dma,
        dma,
        dma((2, 2, half)),
        dma((2, 2, half)),
        dma((2, half)),
        dma((2, half)),
        dma((2, NS)),
        dma((2, NS)),
        dma((heads,)),
        dma((heads,)),
        dma((2, nb // 2, ch)),
        dma((2, nb // 2, ch)),
        dma((heads,)),
        dma((heads,)),
        dma((NH,)),
        dma((NH,)),
        dma((NH,)),
        dma((NH,)),
        dma((half,)),
        dma((half,)),
        dma((2 * half,)),
        dma((half,)),
        dma((3, NS)),
        dma((3, NS)),
        *[pltpu.SemaphoreType.REGULAR] * 5,
    ]
    return pl.pallas_call(
        functools.partial(kernel, NG, NS, NH),
        name="layer",
        out_shape=(
            jax.ShapeDtypeStruct((rows, model), BF),
            jax.ShapeDtypeStruct((rows, qheads * HEAD_WIDTH), BF),
        ),
        in_specs=[hbm, hbm, hbm, hbm, hbm, vmem, vmem, smem, vmem, vmem, vmem, vmem, vmem, hbm, vmem, hbm, hbm],
        out_specs=(hbm, vmem),
        scratch_shapes=scratch,
        compiler_params=pltpu.CompilerParams(
            collective_id=0, has_side_effects=True, vmem_limit_bytes=56 * 1024 * 1024
        ),
    )(
        residual,
        query_in,
        key_in,
        value_in,
        gating_in,
        beta_logit.T,
        decay_logit.T,
        seq_length,
        conv_query,
        conv_key,
        conv_value,
        decay_rate.reshape(-1, 1),
        norm_gain.reshape(1, -1),
        out_weight,
        attn_gain.reshape(1, -1),
        query_weight,
        key_value_weight,
    )


def solution(mesh):
    placed = (
        P(("groups", "seq"), None),
        P(("groups", "seq"), "head"),
        P(("groups", "seq"), "head"),
        P(("groups", "seq"), "head"),
        P(("groups", "seq"), "head"),
        P(("groups", "seq"), "head"),
        P(("groups", "seq"), "head"),
        P("groups"),
        P(None, "head"),
        P(None, "head"),
        P(None, "head"),
        P("head"),
        P(),
        P("head", None),
        P(),
        P("seq", "head"),
        P("seq", None),
    )
    return jax.shard_map(
        functools.partial(shards, mesh.shape["groups"], mesh.shape["seq"], mesh.shape["head"]),
        mesh=mesh,
        in_specs=placed,
        out_specs=(P(("groups", "seq"), None), P(("groups", "seq"), "head")),
        check_vma=False,
    )
```
